32 devices in a mesh: dev: 32 (over z, y, x, core).
Axes of the slice: x: 2, y: 2, z: 4, core: 2. Of those that a mesh axis runs over, the one named last changes fastest.
Arguments:
- tokens: bfloat16 [4608, 1536], P('dev'), may hold values from -6 to 6
- conditioning: bfloat16 [4, 1536], replicated, may hold values from -5 to 5
- text_lengths: int32 [4], replicated, may hold values from 86 to 154, as said below
- modulation_weight: bfloat16 [3072, 9216], P('dev'), may hold values from -0.15625 to 0.15625
- project_weight: bfloat16 [3072, 4608], P('dev'), may hold values from -1 to 1
- merge_weight: bfloat16 [3072, 1536], P('dev'), may hold values from -1.25 to 1.25
- up_weight: bfloat16 [3072, 6144], P('dev'), may hold values from -0.15625 to 0.15625
- down_weight: bfloat16 [12288, 1536], P('dev'), may hold values from -0.078125 to 0.078125
- cotangent: bfloat16 [4608, 1536], P('dev'), may hold values from -6 to 6
Outputs:
- layer_out: bfloat16 [4608, 1536], P('dev')
- tokens_grad: float32 [4608, 1536], P('dev')
- conditioning_grad: float32 [4, 1536], replicated
- modulation_grad: float32 [3072, 9216], P('dev')
- project_grad: float32 [3072, 4608], P('dev')
- merge_grad: float32 [3072, 1536], P('dev')
- up_grad: float32 [3072, 6144], P('dev')
- down_grad: float32 [12288, 1536], P('dev')
The draws below stay inside these ranges and needn't reach their ends.
Inputs may be any that keep to these rules, and one draw needn't show every extreme that they name: `text_lengths`: the text tokens of all sequences sum to 512, so that the sequences fill the packed rows exactly; one sequence has exactly 154 text tokens.
All inputs are finite; a program needn't handle non-finite values.
Results may differ from the reference program's by a relative error of at most 0.025.
The reference program's roundings to bfloat16 on the way count: a program that leaves them out, or rounds other values in their place, can miss the bound.
Values may be sent and summed in bfloat16 or wider, within the bound.
A program may use at most 576 MiB of HBM per device.

```python
import jax
import jax.numpy as jnp
from jax import lax

D = 1536
HEADS = 24
HDIM = 64
FF = 6144
IMG = 1024
TXT = 154
TOKENS = 4608
SEQS = 4


def draw_tokens(key, part):
    noise = jax.random.normal(jax.random.fold_in(key, 101), (TOKENS, D), jnp.float32)
    values = noise
    return jnp.clip(values, -6.0, 6.0).astype(jnp.bfloat16)


def draw_project_weight(key, part):
    base = jax.random.normal(jax.random.fold_in(key, 107), (2 * D, 3 * D), jnp.float32)
    values = jnp.clip(base, -6.0, 6.0) * D ** (-0.5)
    return values.astype(jnp.bfloat16)


def draw_text_lengths(key, part):
    remaining = TOKENS - SEQS * IMG - TXT
    others = SEQS - 1
    base_len = remaining // others
    extra_count = remaining % others
    spread_max = max(1, min(TXT - base_len - 1, base_len - 1, 48))
    key_bumps = jax.random.fold_in(key, 11)
    key_pick = jax.random.fold_in(key, 23)
    bump_vals = jax.random.randint(key_bumps, (others,), 0, spread_max)
    slot_index = jnp.arange(others, dtype=jnp.int32)
    bump_vals = jnp.where(slot_index == 0, 0, jnp.where(slot_index == 1, spread_max - 1, bump_vals)).astype(jnp.int32)
    text_vals = base_len + (slot_index >= others - extra_count).astype(jnp.int32) + bump_vals - jnp.roll(bump_vals, -1)
    pick_index = jax.random.randint(key_pick, (), 0, SEQS)
    seq_index = jnp.arange(SEQS, dtype=jnp.int32)
    from_left = text_vals[jnp.clip(seq_index, 0, others - 1)]
    from_right = text_vals[jnp.clip(seq_index - 1, 0, others - 1)]
    chosen = jnp.where(seq_index < pick_index, from_left, jnp.where(seq_index == pick_index, TXT, from_right))
    return chosen.astype(jnp.int32)


def block_levels(key, extent, cuts, smallest, high):
    loudness, own = 1.0, jax.random.fold_in(key, 6)
    for axis_at, shards_of in cuts:
        heights = jnp.exp(jax.random.uniform(jax.random.fold_in(own, axis_at), (shards_of,), jnp.float32, smallest / len(cuts), high / len(cuts)))
        loudness = loudness * jnp.repeat(heights, extent[axis_at] // shards_of).reshape([-1 if axis == axis_at else 1 for axis in range(len(extent))])
    return loudness


def normal_values(stream_key, extent, deviation, bound, cuts=(), held_as=jnp.bfloat16):
    loudness = block_levels(stream_key, extent, cuts, -0.22, 0.18) if cuts else 1.0
    drawn = jax.random.normal(stream_key, extent, jnp.float32) * deviation * loudness
    return jnp.minimum(jnp.maximum(drawn, -bound), bound).astype(held_as)


def setup_inputs(seed: int = 0) -> dict:
    key_list = jax.random.split(jax.random.key(seed), 10)
    return {
        "tokens": draw_tokens(jax.random.fold_in(key_list[9], 71), 0),
        "conditioning": normal_values(key_list[1], (SEQS, D), 1.0, 5.0),
        "text_lengths": draw_text_lengths(jax.random.fold_in(key_list[9], 71), 0),
        "modulation_weight": normal_values(key_list[3], (2 * D, 6 * D), D ** -0.5, 0.15625, ((0, 32),)),
        "project_weight": draw_project_weight(jax.random.fold_in(key_list[9], 71), 0),
        "merge_weight": normal_values(key_list[5], (2 * D, D), (D // 64) ** -0.5, 1.25, ((0, 32),)),
        "up_weight": normal_values(key_list[6], (2 * D, FF), D ** -0.5, 0.15625, ((0, 32),)),
        "down_weight": normal_values(key_list[7], (2 * FF, D), FF ** -0.5, 0.078125, ((0, 32),)),
        "cotangent": normal_values(key_list[8], (TOKENS, D), 1.0, 6.0, ((0, 32),)),
    }


HIGHEST_PRECISION = lax.Precision.HIGHEST
EPSILON = 1e-06

@jax.custom_vjp
def low(v):
    return lax.optimization_barrier(v.astype(jnp.bfloat16)).astype(jnp.float32)

@jax.custom_vjp
def low_back(v):
    return v

def low_keep(v):
    return (low(v), None)

def low_pass(kept, grad):
    return (grad,)

def back_keep(v):
    return (v, None)

def back_low(kept, grad):
    return (low(grad),)
low.defvjp(low_keep, low_pass)
low_back.defvjp(back_keep, back_low)

def layer_norm(values):
    mean = lax.optimization_barrier(jnp.mean(values, axis=-1, keepdims=True))
    centred = values - mean
    variance = lax.optimization_barrier(jnp.mean(centred * centred, axis=-1, keepdims=True))
    return centred * lax.rsqrt(variance + EPSILON)

def two_streams(rows, weight_pair):
    image_part = jnp.dot(rows[:IMG], weight_pair[0], precision=HIGHEST_PRECISION, preferred_element_type=jnp.float32)
    text_part = jnp.dot(rows[IMG:], weight_pair[1], precision=HIGHEST_PRECISION, preferred_element_type=jnp.float32)
    return jnp.concatenate([image_part, text_part], axis=0)

def sequence_layer(rows, mods, text_count, weights):
    project_pair, merge_pair, up_pair, down_pair = weights
    length = IMG + TXT
    row_index = jnp.arange(length, dtype=jnp.int32)
    is_text = (row_index >= IMG)[:, None]
    mod_rows = jnp.where(is_text, mods[1][None, :], mods[0][None, :])
    shift_a, scale_a, gate_a, shift_b, scale_b, gate_b = jnp.split(mod_rows, 6, axis=1)
    hidden_a = low(layer_norm(rows) * (1.0 + scale_a) + shift_a)
    projected = low_back(low(two_streams(hidden_a, project_pair)))
    queries, keys, values = jnp.split(projected, 3, axis=1)
    queries = queries.reshape(length, HEADS, HDIM)
    keys = keys.reshape(length, HEADS, HDIM)
    values = values.reshape(length, HEADS, HDIM)
    scores = jnp.einsum('qhd,khd->hqk', queries, keys, precision=HIGHEST_PRECISION) * HDIM ** (-0.5)
    scores = low_back(scores)
    key_valid = row_index < IMG + text_count
    masked = jnp.where(key_valid[None, None, :], scores, -jnp.inf)
    top = lax.optimization_barrier(jnp.max(masked, axis=-1, keepdims=True))
    exponent = jnp.exp(masked - top)
    probs = exponent / lax.optimization_barrier(jnp.sum(exponent, axis=-1, keepdims=True))
    attended = jnp.einsum('hqk,khd->qhd', low(probs), values, precision=HIGHEST_PRECISION).reshape(length, HEADS * HDIM)
    attended = low_back(low(attended))
    merged = low_back(two_streams(attended, merge_pair))
    middle = rows + gate_a * merged
    hidden_b = low(layer_norm(middle) * (1.0 + scale_b) + shift_b)
    upper = low_back(two_streams(hidden_b, up_pair))
    activated = low(jax.nn.gelu(upper, approximate=True))
    lowered = low_back(two_streams(activated, down_pair))
    return middle + gate_b * lowered

def reference(tokens, conditioning, text_lengths, modulation_weight, project_weight, merge_weight, up_weight, down_weight, cotangent):
    lengths = text_lengths.astype(jnp.int32)
    ends = jnp.cumsum(IMG + lengths).astype(jnp.int32)
    starts = jnp.concatenate([jnp.zeros((1,), jnp.int32), ends[:-1]])

    def forward(tokens_float, cond_float, mod_flat, project_flat, merge_flat, up_flat, down_flat):
        mod_pair = mod_flat.reshape(2, D, 6 * D)
        project_pair = project_flat.reshape(2, D, 3 * D)
        merge_pair = merge_flat.reshape(2, D, D)
        up_pair = up_flat.reshape(2, D, FF)
        down_pair = down_flat.reshape(2, FF, D)
        silu_low = low(jax.nn.silu(cond_float))
        mods = low_back(jnp.einsum('sd,jdc->sjc', silu_low, mod_pair, precision=HIGHEST_PRECISION))
        padded = jnp.concatenate([tokens_float, jnp.zeros((IMG + TXT, D), jnp.float32)], axis=0)
        layer_fn = jax.checkpoint(sequence_layer)

        def apply_one(carry, seq_index):
            start = starts[seq_index]
            rows = lax.dynamic_slice_in_dim(padded, start, IMG + TXT, 0)
            result = layer_fn(rows, mods[seq_index], lengths[seq_index], (project_pair, merge_pair, up_pair, down_pair))
            return (lax.dynamic_update_slice_in_dim(carry, result, start, 0), None)
        final, unused = lax.scan(apply_one, padded, jnp.arange(SEQS, dtype=jnp.int32))
        return final[:TOKENS]
    output, pullback = jax.vjp(forward, tokens.astype(jnp.float32), conditioning.astype(jnp.float32), modulation_weight.astype(jnp.float32), project_weight.astype(jnp.float32), merge_weight.astype(jnp.float32), up_weight.astype(jnp.float32), down_weight.astype(jnp.float32))
    grads = pullback(cotangent.astype(jnp.float32))
    return (output.astype(jnp.bfloat16), grads[0], grads[1], grads[2], grads[3], grads[4], grads[5], grads[6])
```

```python
import jax
import jax.numpy as jnp
from jax import lax
from jax.experimental import pallas as pl
from jax.experimental.pallas import tpu as pltpu
from jax.sharding import Mesh
from jax.sharding import PartitionSpec as P

HEADS = 24
HDIM = 64
IMG = 1024
RANKS = 8
TXT_PAD = 256
SEQ = IMG + TXT_PAD
IMG_ROWS = IMG // RANKS
TXT_ROWS = TXT_PAD // RANKS
CHUNK = IMG_ROWS + TXT_ROWS
RANK_HEADS = HEADS // RANKS
HEAD_COLS = RANK_HEADS * HDIM
Q_BLOCK = 256
EPSILON = 1e-06
CONTRACT_LAST = (((1,), (1,)), ((), ()))
CONTRACT_FIRST = (((0,), (0,)), ((), ()))
CORES = 2
ALL = ("h", "u", "p", "c")
HALF = ("u", "p", "c")
PLANES = ("h", "u")
RANK = ("p", "c")
HALF_CHIPS = ("u", "p")
LINE = 4
BF = jnp.bfloat16
F32 = jnp.float32


def dot(a, b):
    return jnp.dot(a, b, preferred_element_type=F32)


def dot_last(a, b):
    return lax.dot_general(a, b, CONTRACT_LAST, preferred_element_type=F32)


def dot_first(a, b):
    return lax.dot_general(a, b, CONTRACT_FIRST, preferred_element_type=F32)


def swap(x, axes):
    return lax.all_to_all(x, axes, 0, 0, tiled=True)


def to_all(x, axes):
    count = 1
    for axis in axes:
        count *= lax.axis_size(axis)
    return swap(jnp.broadcast_to(x[None], (count,) + x.shape), axes)


def layer_norm(values):
    mean = jnp.mean(values, axis=-1, keepdims=True)
    centred = values - mean
    variance = jnp.mean(centred * centred, axis=-1, keepdims=True)
    inv_std = lax.rsqrt(variance + EPSILON)
    return (centred * inv_std, inv_std)


def norm_back(grad_normed, normed, inv_std):
    mean_grad = jnp.mean(grad_normed, axis=-1, keepdims=True)
    mean_cross = jnp.mean(grad_normed * normed, axis=-1, keepdims=True)
    return inv_std * (grad_normed - mean_grad - normed * mean_cross)


def attention_forward_body(length_ref, qkv_ref, out_ref, log_ref):
    rows = pl.ds(pl.multiple_of(pl.program_id(0) * Q_BLOCK, Q_BLOCK), Q_BLOCK)
    key_ok = lax.broadcasted_iota(jnp.int32, (Q_BLOCK, SEQ), 1) < length_ref[0]
    for head in range(RANK_HEADS):
        cols = slice(head * HDIM, (head + 1) * HDIM)
        key_cols = slice(HEAD_COLS + head * HDIM, HEAD_COLS + (head + 1) * HDIM)
        value_cols = slice(2 * HEAD_COLS + head * HDIM, 2 * HEAD_COLS + (head + 1) * HDIM)
        query = qkv_ref[rows, cols] * BF(HDIM ** (-0.5))
        scores = jnp.where(key_ok, dot_last(query, qkv_ref[:, key_cols]), -1e30)
        top = jnp.max(scores, axis=1, keepdims=True)
        exponent = jnp.exp(scores - top)
        total = jnp.sum(exponent, axis=1, keepdims=True)
        probs = (exponent * (1.0 / total)).astype(BF)
        out_ref[:, cols] = dot(probs, qkv_ref[:, value_cols]).astype(BF)
        log_ref[:, head : head + 1] = top + jnp.log(total)


def attention_forward(length, qkv):
    return pl.pallas_call(
        attention_forward_body,
        grid=(SEQ // Q_BLOCK,),
        in_specs=[
            pl.BlockSpec(memory_space=pltpu.SMEM),
            pl.BlockSpec((SEQ, 3 * HEAD_COLS), lambda i: (0, 0)),
        ],
        out_specs=[
            pl.BlockSpec((Q_BLOCK, HEAD_COLS), lambda i: (i, 0)),
            pl.BlockSpec((Q_BLOCK, RANK_HEADS), lambda i: (i, 0)),
        ],
        out_shape=[
            jax.ShapeDtypeStruct((SEQ, HEAD_COLS), BF),
            jax.ShapeDtypeStruct((SEQ, RANK_HEADS), F32),
        ],
        cost_estimate=pl.CostEstimate(
            flops=4 * SEQ * SEQ * HEAD_COLS,
            bytes_accessed=8 * SEQ * HEAD_COLS,
            transcendentals=SEQ * SEQ * RANK_HEADS,
        ),
        name="attention_forward",
    )(length, qkv)


def attention_backward_body(length_ref, qkv_ref, grad_ref, log_ref, out_ref, sums):
    step = pl.program_id(0)
    rows = pl.ds(pl.multiple_of(step * Q_BLOCK, Q_BLOCK), Q_BLOCK)
    scale = HDIM ** (-0.5)

    @pl.when(step == 0)
    def _():
        sums[...] = jnp.zeros_like(sums)

    key_ok = lax.broadcasted_iota(jnp.int32, (Q_BLOCK, SEQ), 1) < length_ref[0]
    for head in range(RANK_HEADS):
        cols = slice(head * HDIM, (head + 1) * HDIM)
        next_cols = slice(HEAD_COLS + head * HDIM, HEAD_COLS + (head + 1) * HDIM)
        last_cols = slice(2 * HEAD_COLS + head * HDIM, 2 * HEAD_COLS + (head + 1) * HDIM)
        query = qkv_ref[rows, cols] * BF(scale)
        keys = qkv_ref[:, next_cols]
        grad = grad_ref[:, cols]
        scores = dot_last(query, keys)
        probs = jnp.where(key_ok, jnp.exp(scores - log_ref[:, head : head + 1]), 0.0)
        grad_probs = dot_last(grad, qkv_ref[:, last_cols])
        inner = jnp.sum(probs * grad_probs, axis=1, keepdims=True)
        grad_scores = (probs * (grad_probs - inner)).astype(BF)
        out_ref[rows, cols] = (dot(grad_scores, keys) * scale).astype(BF)
        sums[:, cols] += dot_first(grad_scores, query)
        sums[:, next_cols] += dot_first(probs.astype(BF), grad)

    @pl.when(step == pl.num_programs(0) - 1)
    def _():
        out_ref[:, HEAD_COLS:] = sums[...].astype(BF)


def attention_backward(length, qkv, grad, logs):
    return pl.pallas_call(
        attention_backward_body,
        grid=(SEQ // Q_BLOCK,),
        in_specs=[
            pl.BlockSpec(memory_space=pltpu.SMEM),
            pl.BlockSpec((SEQ, 3 * HEAD_COLS), lambda i: (0, 0)),
            pl.BlockSpec((Q_BLOCK, HEAD_COLS), lambda i: (i, 0)),
            pl.BlockSpec((Q_BLOCK, RANK_HEADS), lambda i: (i, 0)),
        ],
        out_specs=pl.BlockSpec((SEQ, 3 * HEAD_COLS), lambda i: (0, 0)),
        out_shape=jax.ShapeDtypeStruct((SEQ, 3 * HEAD_COLS), BF),
        scratch_shapes=[pltpu.VMEM((SEQ, 2 * HEAD_COLS), F32)],
        cost_estimate=pl.CostEstimate(
            flops=10 * SEQ * SEQ * HEAD_COLS,
            bytes_accessed=14 * SEQ * HEAD_COLS,
            transcendentals=SEQ * SEQ * RANK_HEADS,
        ),
        name="attention_backward",
    )(length, qkv, grad, logs)


def split_halves(first, image, text):
    return jnp.where(first, text, image).astype(BF), jnp.where(first, image, text)


def own_rows(sequence, rank):
    return jnp.concatenate(
        [
            lax.dynamic_slice_in_dim(sequence, rank * IMG_ROWS, IMG_ROWS, 0),
            lax.dynamic_slice_in_dim(sequence, IMG + rank * TXT_ROWS, TXT_ROWS, 0),
        ],
        axis=0,
    )


def by_stream(chunks):
    width = chunks.shape[-1]
    chunks = chunks.reshape(-1, CHUNK, width)
    return (
        chunks[:, :IMG_ROWS].reshape(-1, width),
        chunks[:, IMG_ROWS:].reshape(-1, width),
    )


def to_chunks(image, text):
    width = image.shape[-1]
    return jnp.concatenate(
        [image.reshape(-1, IMG_ROWS, width), text.reshape(-1, TXT_ROWS, width)], axis=1
    )


def pair_blocks(blocks):
    pairs = blocks.reshape((-1, CORES) + blocks.shape[1:])
    first = lax.axis_index("c") == 0
    keep = jnp.where(first, pairs[:, 0], pairs[:, 1])
    send = jnp.where(first, pairs[:, 1], pairs[:, 0])
    got = lax.ppermute(send, "c", [(0, 1), (1, 0)])
    return (keep.astype(F32) + got.astype(F32)).astype(BF)


def total(parts):
    return jnp.sum(parts.astype(F32), axis=0)


def next_planes(rising, falling, planes):
    return (
        lax.ppermute(rising, PLANES, step_planes(1, planes)),
        lax.ppermute(falling, PLANES, step_planes(-1, planes)),
    )


def exchange_planes(parts, planes, plane):
    got = []
    for by in range(1, planes):
        send = lax.dynamic_index_in_dim(parts, (plane + by) % planes, 0, keepdims=False)
        got.append(lax.ppermute(send, PLANES, [(i, (i + by) % planes) for i in range(planes)]))
    return got


def sum_planes(parts, got, plane):
    result = lax.dynamic_index_in_dim(parts, plane, 0, keepdims=False).astype(F32)
    for piece in got:
        result = result + piece.astype(F32)
    return result


def place_rows(sequence, place, halo, count):
    zeros = jnp.zeros((2 * halo, sequence.shape[1]), sequence.dtype)
    padded = jnp.concatenate([zeros, sequence, zeros])
    return lax.dynamic_slice_in_dim(padded, 2 * halo - place, count + 2 * halo, 0)


def stream_rows(table, image_count, text_count):
    is_text = lax.broadcasted_iota(jnp.int32, (image_count + text_count, 1), 0) >= image_count
    return jnp.where(is_text, table[1][None, :], table[0][None, :])


def stream_sums(rows, image_count):
    return jnp.stack([jnp.sum(rows[:image_count], axis=0), jnp.sum(rows[image_count:], axis=0)])


def step_planes(by, planes):
    return [(i, i + by) for i in range(planes) if 0 <= i + by < planes]


def neighbour_rows(from_before, from_after, rank, rows_dev):
    halo, width = from_before.shape
    spans = -(-halo // rows_dev)
    pad = spans * rows_dev - halo
    zeros = jnp.zeros((rows_dev, width), from_before.dtype)
    front = jnp.concatenate([from_before, jnp.zeros((pad, width), from_before.dtype), zeros])
    back = jnp.concatenate([zeros, jnp.zeros((pad, width), from_after.dtype), from_after])
    from_end = RANKS - 1 - rank
    front_at = jnp.minimum(rank, spans) * rows_dev
    back_at = (spans - jnp.minimum(from_end, spans)) * rows_dev
    return lax.dynamic_slice_in_dim(front, front_at, rows_dev, 0) + lax.dynamic_slice_in_dim(
        back, back_at, rows_dev, 0
    )


def layer(
    tokens,
    conditioning,
    text_lengths,
    modulation_weight,
    project_weight,
    merge_weight,
    up_weight,
    down_weight,
    cotangent,
):
    rows_dev, width = tokens.shape
    shard = modulation_weight.shape[0]
    ff_rows = down_weight.shape[0]
    seqs = conditioning.shape[0]
    per_half = lax.axis_size("u")
    planes = 2 * per_half
    half_devices = per_half * RANKS
    devices = 2 * half_devices
    half = lax.axis_index("h")
    rank = lax.axis_index(RANK)
    plane = half * per_half + lax.axis_index("u")
    device = plane * RANKS + rank
    group_rows = RANKS * rows_dev
    halo = -(-13 * seqs // 16) * 16
    mod_cols = 6 * width // RANKS
    other_half = [(0, 1), (1, 0)]

    lengths = IMG + text_lengths
    starts = jnp.cumsum(lengths) - lengths
    length = lax.dynamic_index_in_dim(lengths, plane, 0, keepdims=False)
    start = lax.dynamic_index_in_dim(starts, plane, 0, keepdims=False)
    place = halo + start - plane * group_rows
    valid = (jnp.arange(SEQ, dtype=jnp.int32) < length)[:, None]
    length_arg = length.reshape(1)

    group = lax.all_gather(tokens, RANK, axis=0, tiled=True)
    before = lax.ppermute(group[-halo:], PLANES, step_planes(1, planes))
    after = lax.ppermute(group[:halo], PLANES, step_planes(-1, planes))
    extra = SEQ - group_rows
    window = jnp.concatenate([before, group, after, jnp.zeros((extra, width), BF)])
    sequence = lax.dynamic_slice_in_dim(window, place, SEQ, 0)
    sequence = jnp.where(valid, sequence, jnp.zeros_like(sequence))

    mine = project_weight.reshape(shard, 3, RANKS, HEAD_COLS).transpose(2, 0, 1, 3)
    mine = swap(mine.reshape(RANKS, shard, 3 * HEAD_COLS), RANK)
    mine = mine.reshape(RANKS * shard, 3 * HEAD_COLS)
    rising, falling = [mine], [mine]
    if planes <= LINE:
        up, down = next_planes(mine, mine, planes)
        rising.append(up)
        falling.append(down)

    cond_float = conditioning.astype(F32)
    silu_low = jax.nn.silu(cond_float).astype(BF)
    silu_part = lax.dynamic_slice_in_dim(silu_low, device * shard % width, shard, 1)
    mod_part = dot(silu_part, modulation_weight).reshape(devices, mod_cols)
    mod_mine = jnp.sum(swap(mod_part, ALL).reshape(2, half_devices, mod_cols), axis=1)
    mod_mine, rising, falling = lax.optimization_barrier((mod_mine, rising, falling))

    if planes <= LINE:
        up, down = next_planes(rising[-1], falling[-1], planes)
        rising.append(up)
        falling.append(down)

    mods_half = (
        to_all(mod_mine, HALF)
        .reshape(per_half, RANKS, 2, mod_cols)
        .transpose(0, 2, 1, 3)
        .reshape(per_half, 2, 6, width)
    )
    mods_half, rising, falling = lax.optimization_barrier((mods_half, rising, falling))
    mods = lax.dynamic_index_in_dim(mods_half, lax.axis_index("u"), 0, keepdims=False)
    shift_a, scale_a, gate_a, shift_b, scale_b, gate_b = [mods[:, i] for i in range(6)]

    if planes <= LINE:
        for _ in range(planes - 3):
            up, down = next_planes(rising[-1], falling[-1], planes)
            rising.append(up)
            falling.append(down)
        pieces = jnp.stack(rising[:0:-1] + falling)
        project = lax.dynamic_slice_in_dim(pieces, planes - 1 - plane, planes, 0)
    else:
        project = lax.all_gather(mine, PLANES, axis=0, tiled=True)
    project = project.reshape(2 * width, 3 * HEAD_COLS)

    normed_a, inv_a = layer_norm(sequence.astype(F32))
    hidden_a = (
        normed_a * (1.0 + stream_rows(scale_a, IMG, TXT_PAD)) + stream_rows(shift_a, IMG, TXT_PAD)
    ).astype(BF)

    up_own = swap(up_weight.reshape(shard, half_devices, ff_rows).transpose(1, 0, 2), HALF)
    up_own = up_own.reshape(width, ff_rows)
    project, up_own, down_own, hidden_a = lax.optimization_barrier(
        (project, up_own, down_weight, hidden_a)
    )
    project_image, project_text = project[:width], project[width:]
    merge = lax.all_gather(merge_weight, ALL, axis=0, tiled=True)
    merge_image, merge_text = merge[:width], merge[width:]
    up_other = lax.ppermute(up_own, "h", other_half)
    down_other = lax.ppermute(down_own, "h", other_half)
    first = half == 0
    up_image = jnp.where(first, up_own, up_other)
    up_text = jnp.where(first, up_other, up_own)
    down_image = jnp.where(first, down_own, down_other)
    down_text = jnp.where(first, down_other, down_own)

    cot_half = lax.all_gather(cotangent, HALF, axis=0, tiled=True)
    edge = jnp.where(first, cot_half[-halo:], cot_half[:halo])
    edge = lax.ppermute(edge, "h", other_half)
    none = jnp.zeros_like(edge)
    cot_window = jnp.concatenate(
        [
            jnp.where(first, none, edge),
            cot_half,
            jnp.where(first, edge, none),
            jnp.zeros((extra, width), BF),
        ]
    )
    cot_image, cot_text = [], []
    for index in range(per_half):
        seq = half * per_half + index
        at = halo + starts[seq] - half * per_half * group_rows
        text_ok = (jnp.arange(TXT_PAD, dtype=jnp.int32) < text_lengths[seq])[:, None]
        cot_image.append(lax.dynamic_slice_in_dim(cot_window, at, IMG, 0))
        text = lax.dynamic_slice_in_dim(cot_window, at + IMG, TXT_PAD, 0)
        cot_text.append(jnp.where(text_ok, text, jnp.zeros_like(text)))
    low_image = jnp.concatenate(
        [(mods_half[i, 0, 5][None] * cot_image[i].astype(F32)).astype(BF) for i in range(per_half)]
    )
    low_text = jnp.concatenate(
        [(mods_half[i, 1, 5][None] * cot_text[i].astype(F32)).astype(BF) for i in range(per_half)]
    )
    which = lax.axis_index("u")
    cot_rows = jnp.concatenate(
        [
            lax.dynamic_slice_in_dim(
                jnp.concatenate(cot_image), which * IMG + rank * IMG_ROWS, IMG_ROWS, 0
            ),
            lax.dynamic_slice_in_dim(
                jnp.concatenate(cot_text), which * TXT_PAD + rank * TXT_ROWS, TXT_ROWS, 0
            ),
        ]
    ).astype(F32)

    qkv = jnp.concatenate(
        [dot(hidden_a[:IMG], project_image), dot(hidden_a[IMG:], project_text)]
    ).astype(BF)

    attended, logs = attention_forward(length_arg, qkv)

    attended_rows = swap(to_chunks(attended[:IMG], attended[IMG:]), RANK)
    attended_rows = attended_rows.transpose(1, 0, 2).reshape(CHUNK, width)
    merged = jnp.concatenate(
        [dot(attended_rows[:IMG_ROWS], merge_image), dot(attended_rows[IMG_ROWS:], merge_text)]
    )
    token_rows = own_rows(sequence, rank).astype(F32)
    gate_a_rows = stream_rows(gate_a, IMG_ROWS, TXT_ROWS)
    scale_b_rows = 1.0 + stream_rows(scale_b, IMG_ROWS, TXT_ROWS)
    gate_b_rows = stream_rows(gate_b, IMG_ROWS, TXT_ROWS)
    middle = token_rows + gate_a_rows * merged
    normed_b, inv_b = layer_norm(middle)
    hidden_b = (normed_b * scale_b_rows + stream_rows(shift_b, IMG_ROWS, TXT_ROWS)).astype(BF)

    hidden_all = lax.all_gather(hidden_b, HALF, axis=0, tiled=True)
    att_cols = attended_rows.reshape(CHUNK, per_half, RANKS, shard).transpose(2, 0, 1, 3)
    att_cols = swap(att_cols.reshape(RANKS, CHUNK, per_half * shard), RANK)
    hidden_all, att_cols = lax.optimization_barrier((hidden_all, att_cols))
    hidden_image, hidden_text = by_stream(hidden_all)

    def feed(hidden, up, down, low):
        upper = dot(hidden, up)
        gelu, pull = jax.vjp(lambda value: jax.nn.gelu(value, approximate=True), upper)
        activated = gelu.astype(BF)
        lowered = dot(activated, down)
        grad_upper = pull(dot_last(low, down))[0].astype(BF)
        grad_hidden = dot_last(grad_upper, up)
        return activated, lowered, grad_upper, grad_hidden

    act_image, lowered_image, gu_image, gh_image = feed(
        hidden_image, up_image, down_image, low_image
    )
    act_text, lowered_text, gu_text, gh_text = feed(hidden_text, up_text, down_text, low_text)

    gh_pair = pair_blocks(to_chunks(gh_image.astype(BF), gh_text.astype(BF)))
    gh_parts = swap(gh_pair, HALF_CHIPS)
    low_pair = pair_blocks(to_chunks(lowered_image.astype(BF), lowered_text.astype(BF)))
    down_send, down_keep = split_halves(
        first, dot_first(act_image, low_image), dot_first(act_text, low_text)
    )
    up_send, up_keep = split_halves(
        first, dot_first(hidden_image, gu_image), dot_first(hidden_text, gu_text)
    )
    gh_parts, down_send, up_send, low_pair = lax.optimization_barrier(
        (gh_parts, down_send, up_send, low_pair)
    )
    grad_hidden_b = total(gh_parts)
    down_got = lax.ppermute(down_send, "h", other_half)
    up_got = lax.ppermute(up_send, "h", other_half)

    grad_scale_b = grad_hidden_b * normed_b
    grad_middle = cot_rows + norm_back(grad_hidden_b * scale_b_rows, normed_b, inv_b)
    grad_gate_a = grad_middle * merged
    grad_merged = (gate_a_rows * grad_middle).astype(BF)
    grad_attended = jnp.concatenate(
        [
            dot_last(grad_merged[:IMG_ROWS], merge_image),
            dot_last(grad_merged[IMG_ROWS:], merge_text),
        ]
    ).astype(BF)
    by_head = swap(grad_attended.reshape(CHUNK, RANKS, HEAD_COLS).transpose(1, 0, 2), RANK)
    by_head, low_pair, grad_merged = lax.optimization_barrier((by_head, low_pair, grad_merged))
    low_parts = swap(low_pair, HALF_CHIPS)
    gm_all = lax.all_gather(grad_merged, RANK, axis=0, tiled=True)
    grad_heads = jnp.concatenate(by_stream(by_head))

    grad_projected = attention_backward(length_arg, qkv, grad_heads, logs)

    part = jnp.concatenate(
        [
            dot_first(hidden_a[:IMG], grad_projected[:IMG]).astype(BF),
            dot_first(hidden_a[IMG:], grad_projected[IMG:]).astype(BF),
        ]
    )
    part = part.reshape(planes, RANKS * shard, 3 * HEAD_COLS)
    part, grad_projected = lax.optimization_barrier((part, grad_projected))
    part_got = exchange_planes(part, planes, plane)

    grad_hidden_a = jnp.concatenate(
        [
            dot_last(grad_projected[:IMG], project_image),
            dot_last(grad_projected[IMG:], project_text),
        ]
    )
    back = norm_back(grad_hidden_a * (1.0 + stream_rows(scale_a, IMG, TXT_PAD)), normed_a, inv_a)
    image_at, text_at = rank * IMG_ROWS, IMG + rank * TXT_ROWS
    mine = own_rows(back, rank) + grad_middle
    back = lax.dynamic_update_slice_in_dim(back, mine[:IMG_ROWS], image_at, 0)
    back = lax.dynamic_update_slice_in_dim(back, mine[IMG_ROWS:], text_at, 0)
    back_window = place_rows(back.astype(BF), place, halo, group_rows)
    ends = halo + group_rows
    blocks = jnp.concatenate(
        [
            back_window[halo:ends].reshape(RANKS, rows_dev, width),
            back_window[:halo].reshape(RANKS, halo // RANKS, width),
            back_window[ends : ends + halo].reshape(RANKS, halo // RANKS, width),
        ],
        axis=1,
    )
    back_pair = pair_blocks(blocks)
    back_pair, low_parts = lax.optimization_barrier((back_pair, low_parts))
    back_parts = swap(back_pair, ("p",))
    back_parts, gm_all, down_got, up_got, low_parts = lax.optimization_barrier(
        (back_parts, gm_all, down_got, up_got, low_parts)
    )
    summed = total(back_parts)
    edges = summed[rows_dev:].reshape(2, halo // RANKS, width)
    to_before = lax.ppermute(edges[0], PLANES, step_planes(-1, planes))
    to_after = lax.ppermute(edges[1], PLANES, step_planes(1, planes))
    to_before, to_after, part_got = lax.optimization_barrier((to_before, to_after, part_got))
    edges = to_all(jnp.stack([to_after, to_before]), RANK)
    edges = edges.reshape(RANKS, 2, halo // RANKS, width).transpose(1, 0, 2, 3)
    edges = edges.reshape(2, halo, width)
    tokens_grad = summed[:rows_dev] + neighbour_rows(edges[0], edges[1], rank, rows_dev)

    lowered = total(low_parts)
    layer_rows = (middle + gate_b_rows * lowered).astype(BF)
    layer_seq = jnp.concatenate(by_stream(lax.all_gather(layer_rows, RANK, axis=0, tiled=True)))
    layer_seq = jnp.where(valid, layer_seq, jnp.zeros_like(layer_seq))
    layer_window = place_rows(layer_seq, place, halo, group_rows)
    to_before = lax.ppermute(layer_window[:halo], PLANES, step_planes(-1, planes))
    to_after = lax.ppermute(
        layer_window[halo + group_rows : 2 * halo + group_rows], PLANES, step_planes(1, planes)
    )
    layer_out = lax.dynamic_slice_in_dim(
        layer_window, halo + rank * rows_dev, rows_dev, 0
    ) + neighbour_rows(to_after, to_before, rank, rows_dev)
    grad_gate_b = cot_rows * lowered

    down_grad = down_keep + down_got.astype(F32)
    up_cols = up_keep + up_got.astype(F32)
    up_grad = swap(up_cols.astype(BF).reshape(half_devices, shard, ff_rows), HALF)
    up_grad = up_grad.transpose(1, 0, 2).reshape(shard, half_devices * ff_rows).astype(F32)

    att_image, att_text = by_stream(att_cols)
    gm_image, gm_text = by_stream(gm_all)
    merge_part = jnp.stack([dot_first(att_image, gm_image), dot_first(att_text, gm_text)])
    merge_part = merge_part.astype(BF).reshape(planes, shard, width)
    merge_grad = sum_planes(merge_part, exchange_planes(merge_part, planes, plane), plane)

    part = sum_planes(part, part_got, plane).astype(BF)
    part = swap(part.reshape(RANKS, shard, 3 * HEAD_COLS), RANK)
    part = part.reshape(RANKS, shard, 3, HEAD_COLS).transpose(1, 2, 0, 3)
    project_grad = part.reshape(shard, 3 * width).astype(F32)

    grads = jnp.stack(
        [
            stream_sums(grad_hidden_a, IMG),
            stream_sums(grad_hidden_a * normed_a, IMG),
            stream_sums(grad_gate_a, IMG_ROWS),
            stream_sums(grad_hidden_b, IMG_ROWS),
            stream_sums(grad_scale_b, IMG_ROWS),
            stream_sums(grad_gate_b, IMG_ROWS),
        ],
        axis=1,
    )
    grads = grads.reshape(2, RANKS, mod_cols).transpose(1, 0, 2)
    grads = jnp.sum(swap(grads, RANK), axis=0).astype(BF)
    own_grads = swap(jnp.repeat(grads, half_devices, axis=0), ALL).reshape(seqs, 6 * width)
    modulation_grad = dot_first(silu_part, own_grads)
    piece = dot_last(own_grads, modulation_weight)
    pieces = to_all(piece, ALL).reshape(2, half_devices, seqs, shard)
    grad_silu = jnp.sum(pieces, axis=0).transpose(1, 0, 2).reshape(seqs, width)
    conditioning_grad = jax.vjp(jax.nn.silu, cond_float)[1](grad_silu)[0]

    return (
        layer_out,
        tokens_grad,
        conditioning_grad,
        modulation_grad,
        project_grad,
        merge_grad,
        up_grad,
        down_grad,
    )


def solution(mesh):
    count = mesh.devices.size
    grid = Mesh(mesh.devices.reshape(2, count // (2 * RANKS), RANKS // CORES, CORES), ALL)
    rows = P(ALL, None)
    return jax.shard_map(
        layer,
        mesh=grid,
        in_specs=(rows, P(), P(), rows, rows, rows, rows, rows, rows),
        out_specs=(rows, rows, P(), rows, rows, rows, rows, rows),
        check_vma=False,
    )
```
